16 devices in a mesh: dp: 2 (over y, z), sp: 8 (over x, core).
Axes of the slice: x: 4, y: 2, z: 1, core: 2. Of those that a mesh axis runs over, the one named last changes fastest.
The devices are a block of a 4x4x8 slice.
Arguments:
- x: bfloat16 [4096, 7168], P(('dp', 'sp')), parts along dimension 0
- gain: bfloat16 [7168], replicated
- wq: bfloat16 [7168, 7168], replicated
- wk: bfloat16 [7168, 7168], replicated
- wv: bfloat16 [7168, 7168], replicated
- wo: bfloat16 [7168, 7168], replicated
Outputs:
- output: bfloat16 [4096, 7168], P(('dp', 'sp')), parts along dimension 0
There are 2 independent parts. The reference program is written for one: setup_inputs(seed, part) draws one part's arguments, and reference() takes and returns one part's arrays. A program takes and returns all parts, laid end to end along the dimension named above; an argument that names none is the same for every part.
All inputs are finite; a program needn't handle non-finite values.
Results may differ from the reference program's by a relative error of at most 0.012.
Values are sent between devices in bfloat16 or wider.
A program may use at most 768 MiB of HBM per device.

```python
import jax
import jax.numpy as jnp
from jax import lax

ROWS = 2048
D = 7168
HEADS = 56
KV_HEADS = 56
HEAD = 128
THETA = 10000


def setup_inputs(seed: int = 0, part: int = 0) -> dict:
    kx, kn, kq, kk, kv, ko = jax.random.split(jax.random.key(seed), 6)

    def weights(key, rows, columns):
        return jax.random.normal(key, (rows, columns), jnp.float32) * rows**-0.5

    drawn = {
        "x": jax.random.normal(jax.random.fold_in(kx, part), (ROWS, D), jnp.float32),
        "gain": 1 + 0.1 * jax.random.normal(kn, (D,), jnp.float32),
        "wq": 2 * weights(kq, D, HEADS * HEAD),
        "wk": 2 * weights(kk, D, KV_HEADS * HEAD),
        "wv": 4 * weights(kv, D, KV_HEADS * HEAD),
        "wo": weights(ko, HEADS * HEAD, D),
    }
    return {k: v.astype(jnp.bfloat16) for k, v in drawn.items()}


def normed(x, gain):
    wide = x.astype(jnp.float32)
    scale = lax.rsqrt(jnp.mean(wide * wide, -1, keepdims=True) + 1e-6)
    return (wide * scale * gain.astype(jnp.float32)).astype(jnp.bfloat16)


def turned(t, place, theta):
    half = t.shape[-1] // 2
    angle = place.astype(jnp.float32)[:, None] * theta ** (-jnp.arange(half, dtype=jnp.float32) / half)
    cos, sin = jnp.cos(angle)[:, None], jnp.sin(angle)[:, None]
    a, b = t[..., :half].astype(jnp.float32), t[..., half:].astype(jnp.float32)
    return jnp.concatenate([a * cos - b * sin, b * cos + a * sin], -1).astype(jnp.bfloat16)


def matmul(a, w):
    return jnp.dot(a, w, preferred_element_type=jnp.float32).astype(jnp.bfloat16)


def einsum(form, a, b):
    return jnp.einsum(form, a.astype(jnp.float32), b.astype(jnp.float32))


def attention(q, k, v):
    scores = einsum("tgsd,ugd->gstu", q, k) * q.shape[-1] ** -0.5
    token = jnp.arange(q.shape[0])
    scores = jnp.where(token[:, None] >= token, scores, -jnp.inf)
    weights = jax.nn.softmax(scores, -1).astype(jnp.bfloat16)
    return einsum("gstu,ugd->tgsd", weights, v).astype(jnp.bfloat16)


def reference(x, gain, wq, wk, wv, wo):
    a, place = normed(x, gain), jnp.arange(ROWS)
    q = turned(matmul(a, wq).reshape(ROWS, HEADS, HEAD), place, THETA).reshape(ROWS, KV_HEADS, -1, HEAD)
    k = turned(matmul(a, wk).reshape(ROWS, KV_HEADS, HEAD), place, THETA)
    v = matmul(a, wv).reshape(ROWS, KV_HEADS, HEAD)
    seen = attention(q, k, v).reshape(ROWS, HEADS * HEAD)
    return (x.astype(jnp.float32) + jnp.dot(seen, wo, preferred_element_type=jnp.float32)).astype(jnp.bfloat16)
```

```python
import functools

import jax
import jax.numpy as jnp
from jax import lax
from jax.experimental import pallas as pl
from jax.experimental.pallas import tpu as pltpu
from jax.sharding import PartitionSpec as P

HEAD = 128
THETA = 10000
LOG2E = 1.4426950408889634
HIDDEN = -2e30
WIDE = 512
RING = 3
LAG = 2
MESH = pl.DeviceIdType.MESH


def _dot(a, b, ca, cb):
    return lax.dot_general(a, b, (((ca,), (cb,)), ((), ())), preferred_element_type=jnp.float32)


def _kernel(n, x_hbm, gain_ref, cos_ref, sin_ref, wq_hbm, wk_hbm, wv_hbm, wo_hbm, y_hbm,
            a_ref, ring, sent, got, mine, seen, total, score, prob, vt,
            x_sem, ring_sem, send_sem, recv_sem, osend_sem, orecv_sem, y_sem):
    own, dim = a_ref.shape
    stages = got.shape[0]
    per = n * HEAD
    halves = per // WIDE
    heads = WIDE // HEAD
    ptiles = 3 * halves
    units = dim // per
    wtiles = dim // WIDE // units
    me = lax.axis_index("sp")
    scale = HEAD**-0.5 * LOG2E

    first_w = LAG + 1
    steps = stages + first_w
    head_tiles = first_w * ptiles
    mid_tiles = head_tiles + (stages - first_w) * (ptiles + wtiles)
    all_tiles = stages * (ptiles + wtiles)

    def fetch_p(slot, stage, i):
        for c, w in enumerate((wq_hbm, wk_hbm, wv_hbm)):
            for h in range(halves):
                @pl.when(i == c * halves + h)
                def _():
                    col = pl.multiple_of(stage * per + h * WIDE, WIDE)
                    pltpu.make_async_copy(w.at[:, pl.ds(col, WIDE)], ring.at[slot], ring_sem.at[slot]).start()

    def fetch_w(slot, stage, j):
        row = pl.multiple_of(stage * per, per)
        for u in range(units):
            col = pl.multiple_of((j * units + u) * WIDE, WIDE)
            pltpu.make_async_copy(wo_hbm.at[pl.ds(row, per), pl.ds(col, WIDE)], ring.at[slot, pl.ds(u * per, per)], ring_sem.at[slot]).start()

    def fetch(at):
        slot = lax.rem(at, RING)
        mid = jnp.maximum(at - head_tiles, 0)
        late = jnp.maximum(at - mid_tiles, 0)
        both = ptiles + wtiles
        in_head, in_mid = at < head_tiles, at < mid_tiles
        is_p = in_head | (in_mid & (lax.rem(mid, both) < ptiles))
        p_stage = jnp.where(in_head, lax.div(at, ptiles), first_w + lax.div(mid, both))
        p_tile = jnp.where(in_head, lax.rem(at, ptiles), lax.rem(mid, both))
        w_stage = jnp.where(in_mid, lax.div(mid, both), stages - first_w + lax.div(late, wtiles))
        w_tile = jnp.where(in_mid, lax.rem(mid, both) - ptiles, lax.rem(late, wtiles))

        @pl.when(is_p)
        def _():
            fetch_p(slot, p_stage, p_tile)

        @pl.when(jnp.logical_not(is_p) & (at < all_tiles))
        def _():
            fetch_w(slot, w_stage, w_tile)

    def arrived(at):
        slot = lax.rem(at, RING)
        pltpu.make_async_copy(wq_hbm.at[:, pl.ds(0, WIDE)], ring.at[slot], ring_sem.at[slot]).wait()
        return slot

    load_x = pltpu.make_async_copy(x_hbm, a_ref, x_sem)
    load_x.start()
    for at in range(RING):
        fetch_p(at, 0, at)

    barrier = pltpu.get_barrier_semaphore()
    for k in range(1, n):
        pl.semaphore_signal(barrier, inc=1, device_id={"sp": lax.rem(me + k, n)}, device_id_type=MESH)

    vt[HEAD:, :] = jnp.ones((vt.shape[0] - HEAD, vt.shape[1]), vt.dtype)
    load_x.wait()
    gain = gain_ref[...].astype(jnp.float32)

    def norm(r, _):
        rows = pl.ds(pl.multiple_of(r * 16, 16), 16)
        wide = a_ref[rows, :].astype(jnp.float32)
        total[rows, :] = wide
        s = lax.rsqrt(jnp.mean(wide * wide, -1, keepdims=True) + 1e-6)
        a_ref[rows, :] = (wide * s * gain).astype(a_ref.dtype)
        return 0

    lax.fori_loop(0, own // 16, norm, 0)
    pl.semaphore_wait(barrier, n - 1)

    def to_peer(stage, slot, c, d):
        return pltpu.make_async_remote_copy(
            src_ref=sent.at[slot, c, d], dst_ref=got.at[stage, c, pl.ds(pl.multiple_of(me * own, own), own)],
            send_sem=send_sem.at[slot, c, d], recv_sem=recv_sem.at[stage, c, me], device_id={"sp": d}, device_id_type=MESH)

    def result(stage, slot, d):
        return pltpu.make_async_remote_copy(
            src_ref=mine.at[slot, pl.ds(d * own, own)], dst_ref=seen.at[stage, :, pl.ds(pl.multiple_of(me * HEAD, HEAD), HEAD)],
            send_sem=osend_sem.at[slot, d], recv_sem=orecv_sem.at[stage, me], device_id={"sp": d}, device_id_type=MESH)

    def base(t):
        return jnp.where(t < first_w, t * ptiles, head_tiles + jnp.minimum(t - first_w, stages - first_w) * (ptiles + wtiles)
                         + jnp.maximum(t - stages, 0) * wtiles)

    def project(t):
        slot = lax.rem(t, 2)

        @pl.when(t >= 2)
        def _():
            for c in range(3):
                for d in range(n):
                    @pl.when(d != me)
                    def _():
                        to_peer(t, slot, c, d).wait_send()

        def tile(i, _):
            at = base(t) + i
            w = arrived(at)
            c, h = lax.div(i, halves), lax.rem(i, halves)
            out = jnp.dot(a_ref[...], ring[w], preferred_element_type=jnp.float32).astype(jnp.bfloat16)

            @pl.when(c < 2)
            def _():
                cos, sin = cos_ref[...], sin_ref[...]
                for e in range(heads):
                    v = out[:, e * HEAD : (e + 1) * HEAD].astype(jnp.float32)
                    sent[slot, c, h * heads + e] = (v * cos + pltpu.roll(v, HEAD // 2, 1) * sin).astype(jnp.bfloat16)

            @pl.when(c == 2)
            def _():
                for e in range(heads):
                    sent[slot, c, h * heads + e] = out[:, e * HEAD : (e + 1) * HEAD]

            fetch(at + RING)
            for e in range(heads):
                d = h * heads + e

                @pl.when(d != me)
                def _():
                    to_peer(t, slot, c, d).start()

                @pl.when(d == me)
                def _():
                    got[t, c, pl.ds(pl.multiple_of(me * own, own), own), :] = sent[slot, c, d]
            return 0

        lax.fori_loop(0, ptiles, tile, 0)

    def attend(s):
        slot = lax.rem(s, 2)
        for c in range(3):
            for d in range(n):
                @pl.when(d != me)
                def _():
                    pltpu.make_async_remote_copy(
                        src_ref=sent.at[0, c, d], dst_ref=got.at[s, c, pl.ds(d * own, own)], send_sem=send_sem.at[0, c, d],
                        recv_sem=recv_sem.at[s, c, d], device_id={"sp": d}, device_id_type=MESH).wait_recv()

        @pl.when(s >= 2)
        def _():
            for d in range(n):
                @pl.when(d != me)
                def _():
                    result(s, slot, d).wait_send()

        for d in range(n):
            here = slice(d * own, (d + 1) * own)
            vt[:HEAD, here] = got[s, 2, here, :].T
        gap = lax.broadcasted_iota(jnp.int32, (own, own), 1) - lax.broadcasted_iota(jnp.int32, (own, own), 0)
        for d in range(n):
            b = d % 2
            q = got[s, 0, d * own : (d + 1) * own, :]
            top = None
            for j in range(d + 1):
                here = slice(j * own, (j + 1) * own)
                one = _dot(got[s, 1, here, :], q, 1, 1)
                if j == d:
                    one = jnp.where(gap >= 0, one, HIDDEN)
                score[b, here, :] = one
                high = one.max(axis=0, keepdims=True)
                top = high if top is None else jnp.maximum(top, high)
            for j in range(d + 1):
                here = slice(j * own, (j + 1) * own)
                prob[b, here, :] = jnp.exp2((score[b, here, :] - top) * scale).astype(jnp.bfloat16)
            till = slice(0, (d + 1) * own)
            mix = _dot(vt[:, till], prob[b, till, :], 1, 0)
            out = (mix[:HEAD] * (1 / mix[HEAD : HEAD + 1])).T.astype(jnp.bfloat16)
            mine[slot, d * own : (d + 1) * own, :] = out

            @pl.when(d != me)
            def _():
                result(s, slot, d).start()

            @pl.when(d == me)
            def _():
                seen[s, :, pl.ds(pl.multiple_of(me * HEAD, HEAD), HEAD)] = mine[slot, d * own : (d + 1) * own, :]

    def finish(t, s):
        for d in range(n):
            @pl.when(d != me)
            def _():
                pltpu.make_async_remote_copy(
                    src_ref=mine.at[0, pl.ds(d * own, own)], dst_ref=seen.at[s, :, pl.ds(d * HEAD, HEAD)],
                    send_sem=osend_sem.at[0, d], recv_sem=orecv_sem.at[s, d], device_id={"sp": d}, device_id_type=MESH).wait_recv()

        def tile(j, _):
            at = base(t) + jnp.where(t < stages, ptiles, 0) + j
            w = arrived(at)
            for u in range(units):
                cols = pl.ds(pl.multiple_of((j * units + u) * WIDE, WIDE), WIDE)
                total[:, cols] += jnp.dot(seen[s], ring[w, u * per : (u + 1) * per, :], preferred_element_type=jnp.float32)
            fetch(at + RING)
            return 0

        lax.fori_loop(0, wtiles, tile, 0)

    def step(t, _):
        @pl.when(t < stages)
        def _():
            project(t)

        @pl.when((t >= LAG) & (t < LAG + stages))
        def _():
            attend(t - LAG)

        @pl.when(t >= first_w)
        def _():
            finish(t, t - first_w)

        return 0

    lax.fori_loop(0, steps, step, 0)

    def store(u, _):
        cols = pl.ds(pl.multiple_of(u * per, per), per)
        a_ref[:, cols] = total[:, cols].astype(a_ref.dtype)
        return 0

    lax.fori_loop(0, units, store, 0)
    out = pltpu.make_async_copy(a_ref, y_hbm, y_sem)
    out.start()
    for slot in range(2):
        for d in range(n):
            @pl.when(d != me)
            def _():
                for c in range(3):
                    to_peer(0, slot, c, d).wait_send()
                result(0, slot, d).wait_send()
    out.wait()


def solution(mesh):
    n = mesh.shape["sp"]

    def body(x, gain, wq, wk, wv, wo):
        own, dim = x.shape
        per = n * HEAD
        stages = dim // per
        half = HEAD // 2
        place = lax.axis_index("sp") * own + jnp.arange(own)
        angle = place.astype(jnp.float32)[:, None] * THETA ** (-jnp.arange(half, dtype=jnp.float32) / half)
        cos, sin = jnp.cos(angle), jnp.sin(angle)
        cos, sin = jnp.concatenate([cos, cos], 1), jnp.concatenate([-sin, sin], 1)
        tokens = n * own
        low = jnp.bfloat16
        hbm = pl.BlockSpec(memory_space=pl.ANY)
        vmem = pl.BlockSpec(memory_space=pltpu.VMEM)
        return pl.pallas_call(
            functools.partial(_kernel, n),
            out_shape=jax.ShapeDtypeStruct((own, dim), low),
            in_specs=[hbm, vmem, vmem, vmem, hbm, hbm, hbm, hbm],
            out_specs=hbm,
            scratch_shapes=[
                pltpu.VMEM((own, dim), low),
                pltpu.VMEM((RING, dim, WIDE), low),
                pltpu.VMEM((2, 3, n, own, HEAD), low),
                pltpu.VMEM((stages, 3, tokens, HEAD), low),
                pltpu.VMEM((2, tokens, HEAD), low),
                pltpu.VMEM((stages, own, per), low),
                pltpu.VMEM((own, dim), jnp.float32),
                pltpu.VMEM((2, tokens, own), jnp.float32),
                pltpu.VMEM((2, tokens, own), low),
                pltpu.VMEM((HEAD + 16, tokens), low),
                pltpu.SemaphoreType.DMA,
                pltpu.SemaphoreType.DMA((RING,)),
                pltpu.SemaphoreType.DMA((2, 3, n)),
                pltpu.SemaphoreType.DMA((stages, 3, n)),
                pltpu.SemaphoreType.DMA((2, n)),
                pltpu.SemaphoreType.DMA((stages, n)),
                pltpu.SemaphoreType.DMA,
            ],
            compiler_params=pltpu.CompilerParams(collective_id=0, has_side_effects=True, vmem_limit_bytes=67043328),
            name="layer",
        )(x, gain[None], cos, sin, wq, wk, wv, wo)

    tokens, whole = P(("dp", "sp"), None), P(None, None)
    return jax.shard_map(
        body,
        mesh=mesh,
        in_specs=(tokens, P(None), whole, whole, whole, whole),
        out_specs=tokens,
        check_vma=False,
    )
```

```python
import functools

import jax
import jax.numpy as jnp
import numpy as np
from jax import lax
from jax.experimental import pallas as pl
from jax.experimental.pallas import tpu as pltpu
from jax.sharding import PartitionSpec as P

HEAD = 128
THETA = 10000
LOG2E = 1.4426950408889634
HIDDEN = -2e30
WIDE = 512
RING = 3
LAG = 1
STRIP = 512
PIECE = 64
ROWS = 64
MESH = pl.DeviceIdType.MESH


def _dot(a, b, ca, cb):
    return lax.dot_general(a, b, (((ca,), (cb,)), ((), ())), preferred_element_type=jnp.float32)


def _kernel(n, x_hbm, gain_ref, table_hbm, wq_hbm, wk_hbm, wv_hbm, wo_hbm, y_ref,
            a_ref, ring, sent, got, mine, seen, total, score, prob, vt, raw, table, turns,
            x_sem, table_sem, ring_sem, send_sem, recv_sem, osend_sem, orecv_sem):
    own, dim = a_ref.shape
    stages = got.shape[0]
    per = n * HEAD
    halves = per // WIDE
    heads = WIDE // HEAD
    ptiles = 3 * halves
    units = dim // per
    wtiles = dim // WIDE // units
    me = lax.axis_index("sp")
    scale = HEAD**-0.5 * LOG2E

    first_w = LAG + 1
    steps = stages + first_w
    head_tiles = first_w * ptiles
    mid_tiles = head_tiles + (stages - first_w) * (ptiles + wtiles)
    all_tiles = stages * (ptiles + wtiles)

    def fetch_p(slot, stage, i):
        for c, w in enumerate((wq_hbm, wk_hbm, wv_hbm)):
            for h in range(halves):
                @pl.when(i == c * halves + h)
                def _():
                    col = pl.multiple_of(stage * per + h * WIDE, WIDE)
                    pltpu.make_async_copy(w.at[:, pl.ds(col, WIDE)], ring.at[slot], ring_sem.at[slot]).start()

    def fetch_w(slot, stage, j):
        row = pl.multiple_of(stage * per, per)
        for u in range(units):
            col = pl.multiple_of((j * units + u) * WIDE, WIDE)
            pltpu.make_async_copy(wo_hbm.at[pl.ds(row, per), pl.ds(col, WIDE)], ring.at[slot, pl.ds(u * per, per)], ring_sem.at[slot]).start()

    def fetch(at):
        slot = lax.rem(at, RING)
        mid = jnp.maximum(at - head_tiles, 0)
        late = jnp.maximum(at - mid_tiles, 0)
        both = ptiles + wtiles
        in_head, in_mid = at < head_tiles, at < mid_tiles
        is_p = in_head | (in_mid & (lax.rem(mid, both) < ptiles))
        p_stage = jnp.where(in_head, lax.div(at, ptiles), first_w + lax.div(mid, both))
        p_tile = jnp.where(in_head, lax.rem(at, ptiles), lax.rem(mid, both))
        w_stage = jnp.where(in_mid, lax.div(mid, both), stages - first_w + lax.div(late, wtiles))
        w_tile = jnp.where(in_mid, lax.rem(mid, both) - ptiles, lax.rem(late, wtiles))

        @pl.when(is_p)
        def _():
            fetch_p(slot, p_stage, p_tile)

        @pl.when(jnp.logical_not(is_p) & (at < all_tiles))
        def _():
            fetch_w(slot, w_stage, w_tile)

    def arrived(at):
        slot = lax.rem(at, RING)
        pltpu.make_async_copy(wq_hbm.at[:, pl.ds(0, WIDE)], ring.at[slot], ring_sem.at[slot]).wait()
        return slot

    load_x = pltpu.make_async_copy(x_hbm, a_ref, x_sem)
    load_x.start()
    load_turns = pltpu.make_async_copy(table_hbm.at[pl.ds(pl.multiple_of(me * own, own), own)], turns, table_sem)
    load_turns.start()
    for at in range(RING):
        fetch_p(at, 0, at)

    barrier = pltpu.get_barrier_semaphore()
    for k in range(1, n):
        pl.semaphore_signal(barrier, inc=1, device_id={"sp": lax.rem(me + k, n)}, device_id_type=MESH)

    vt[HEAD:, :] = jnp.ones((vt.shape[0] - HEAD, vt.shape[1]), vt.dtype)

    def clear(u, _):
        total[:, pl.ds(pl.multiple_of(u * WIDE, WIDE), WIDE)] = jnp.zeros((own, WIDE), jnp.float32)
        return 0

    lax.fori_loop(0, dim // WIDE, clear, 0)
    load_turns.wait()
    both_parts = turns[...]
    swapped = pltpu.roll(both_parts, HEAD // 2, 1)
    first = lax.broadcasted_iota(jnp.int32, both_parts.shape, 1) < HEAD // 2
    table[0, 0] = jnp.where(first, both_parts, swapped)
    table[0, 1] = jnp.where(first, -swapped, both_parts)
    table[1, 0] = jnp.ones_like(both_parts)
    table[1, 1] = jnp.zeros_like(both_parts)
    load_x.wait()

    def norm(r, _):
        rows = pl.ds(pl.multiple_of(r * ROWS, ROWS), ROWS)
        squares = jnp.zeros((ROWS, HEAD), jnp.float32)
        for c in range(0, dim, HEAD):
            wide = a_ref[rows, c : c + HEAD].astype(jnp.float32)
            squares += wide * wide
        s = lax.rsqrt(squares.sum(-1, keepdims=True) / dim + 1e-6)
        s = jnp.broadcast_to(s, (ROWS, HEAD))
        for c in range(0, dim, HEAD):
            wide = a_ref[rows, c : c + HEAD].astype(jnp.float32)
            a_ref[rows, c : c + HEAD] = (wide * s * gain_ref[pl.ds(c, HEAD)].astype(jnp.float32).reshape(1, HEAD)).astype(a_ref.dtype)
        return 0

    lax.fori_loop(0, own // ROWS, norm, 0)
    pl.semaphore_wait(barrier, n - 1)

    def to_peer(stage, slot, c, d):
        return pltpu.make_async_remote_copy(
            src_ref=sent.at[slot, c, d], dst_ref=got.at[stage, c, pl.ds(pl.multiple_of(me * own, own), own)],
            send_sem=send_sem.at[slot, c, d], recv_sem=recv_sem.at[stage, c, me], device_id={"sp": d}, device_id_type=MESH)

    def result(stage, slot, d):
        return pltpu.make_async_remote_copy(
            src_ref=mine.at[slot, pl.ds(pl.multiple_of(d * own, own), own)], dst_ref=seen.at[stage, :, pl.ds(pl.multiple_of(me * HEAD, HEAD), HEAD)],
            send_sem=osend_sem.at[slot, d], recv_sem=orecv_sem.at[stage, me], device_id={"sp": d}, device_id_type=MESH)

    def base(t):
        return jnp.where(t < first_w, t * ptiles, head_tiles + jnp.minimum(t - first_w, stages - first_w) * (ptiles + wtiles)
                         + jnp.maximum(t - stages, 0) * wtiles)

    def project(t):
        slot = lax.rem(t, 2)

        @pl.when(t >= 2)
        def _():
            for c in range(3):
                for k in range(1, n):
                    to_peer(t, slot, c, lax.rem(me + k, n)).wait_send()

        def turn(c, h, to):
            for e in range(heads):
                v = raw[:, e * HEAD : (e + 1) * HEAD].astype(jnp.float32)
                cos, sin = table[lax.div(c, 2), 0], table[lax.div(c, 2), 1]
                sent[slot, to, h * heads + e] = (v * cos + pltpu.roll(v, HEAD // 2, 1) * sin).astype(jnp.bfloat16)

        def send(c, h):
            for e in range(heads):
                d = h * heads + e

                @pl.when(d != me)
                def _():
                    to_peer(t, slot, c, d).start()

        def tile(i, _):
            at = base(t) + i
            w = arrived(at)
            before = jnp.maximum(i - 1, 0)
            c, h = lax.div(before, halves), lax.rem(before, halves)
            turn(c, h, jnp.where((i == 1) & (t == 0), 2, c))
            raw[...] = jnp.dot(a_ref[...], ring[w], preferred_element_type=jnp.float32).astype(jnp.bfloat16)
            fetch(at + RING)

            @pl.when(i > 1 - jnp.minimum(t, 1))
            def _():
                send(c, h)

            @pl.when((i == 0) & (t == 0))
            def _():
                turn(0, 0, 0)
                send(0, 0)

            return 0

        lax.fori_loop(0, ptiles, tile, 0)
        turn(2, halves - 1, 2)
        send(2, halves - 1)
        for c in range(3):
            got[t, c, pl.ds(pl.multiple_of(me * own, own), own), :] = sent[slot, c, me]

    def attend(s):
        slot = lax.rem(s, 2)
        for c in range(3):
            for k in range(1, n):
                d = lax.rem(me + k, n)
                pltpu.make_async_remote_copy(
                    src_ref=sent.at[0, c, d], dst_ref=got.at[s, c, pl.ds(pl.multiple_of(d * own, own), own)], send_sem=send_sem.at[0, c, d],
                    recv_sem=recv_sem.at[s, c, d], device_id={"sp": d}, device_id_type=MESH).wait_recv()

        @pl.when(s >= 2)
        def _():
            for k in range(1, n):
                result(s, slot, lax.rem(me + k, n)).wait_send()

        tokens = n * own
        strips = tokens // STRIP
        for j in range(strips):
            here = slice(j * STRIP, (j + 1) * STRIP)
            vt[:HEAD, here] = got[s, 2, here, :].T
        gap = lax.broadcasted_iota(jnp.int32, (PIECE, STRIP), 1) - lax.broadcasted_iota(jnp.int32, (PIECE, STRIP), 0)

        def scores(i, j, top):
            q = got[s, 0, i * STRIP : (i + 1) * STRIP, :]
            one = _dot(got[s, 1, j * STRIP : (j + 1) * STRIP, :], q, 1, 1)
            for p in range(0, STRIP, PIECE):
                part = one[p : p + PIECE]
                if i == j:
                    part = jnp.where(gap >= p, part, HIDDEN)
                score[j * STRIP + p : j * STRIP + p + PIECE, :] = part
                high = part.reshape(PIECE // 8, 8, STRIP).max(axis=0)
                top = high if top is None else jnp.maximum(top, high)
            return top

        def weights(j, top):
            for p in range(j * STRIP, (j + 1) * STRIP, PIECE):
                prob[p : p + PIECE, :] = jnp.exp2((score[p : p + PIECE, :] - top) * scale).astype(jnp.bfloat16)

        def values(i):
            till = (i + 1) * STRIP
            mix = _dot(vt[:, :till], prob[:till, :], 1, 0)
            mine[slot, i * STRIP : till, :] = (mix[:HEAD] * (1 / mix[HEAD : HEAD + 1])).T.astype(jnp.bfloat16)

        top = scores(0, 0, None)
        for i in range(strips):
            top, after = top.max(axis=0, keepdims=True), None
            for j in range(i + 1):
                weights(j, top)
                if i + 1 < strips:
                    after = scores(i + 1, j, after)
            if i + 1 < strips:
                after = scores(i + 1, i + 1, after)
            values(i)
            top = after

        for d in range(n):
            @pl.when(d != me)
            def _():
                result(s, slot, d).start()
        seen[s, :, pl.ds(pl.multiple_of(me * HEAD, HEAD), HEAD)] = mine[slot, pl.ds(pl.multiple_of(me * own, own), own), :]

    def finish(t, s):
        for k in range(1, n):
            d = lax.rem(me + k, n)
            pltpu.make_async_remote_copy(
                src_ref=mine.at[0, pl.ds(0, own)], dst_ref=seen.at[s, :, pl.ds(pl.multiple_of(d * HEAD, HEAD), HEAD)],
                send_sem=osend_sem.at[0, d], recv_sem=orecv_sem.at[s, d], device_id={"sp": d}, device_id_type=MESH).wait_recv()

        def tile(j, _):
            at = base(t) + jnp.where(t < stages, ptiles, 0) + j
            w = arrived(at)
            for u in range(units):
                cols = pl.ds(pl.multiple_of((j * units + u) * WIDE, WIDE), WIDE)
                total[:, cols] += jnp.dot(seen[s], ring[w, u * per : (u + 1) * per, :], preferred_element_type=jnp.float32)
            fetch(at + RING)
            return 0

        lax.fori_loop(0, wtiles, tile, 0)

    def step(t, _):
        @pl.when(t < stages)
        def _():
            project(t)

        @pl.when((t >= LAG) & (t < LAG + stages))
        def _():
            attend(t - LAG)

        @pl.when(t == stages)
        def _():
            load_x.start()

        @pl.when(t >= first_w)
        def _():
            finish(t, t - first_w)

        return 0

    lax.fori_loop(0, steps, step, 0)

    load_x.wait()
    for u in range(units):
        cols = slice(u * per, (u + 1) * per)

        def store(r, _):
            rows = pl.ds(pl.multiple_of(r * ROWS, ROWS), ROWS)
            y_ref[rows, cols] = (a_ref[rows, cols].astype(jnp.float32) + total[rows, cols]).astype(a_ref.dtype)
            return 0

        lax.fori_loop(0, own // ROWS, store, 0)
    for slot in range(2):
        for k in range(1, n):
            d = lax.rem(me + k, n)
            for c in range(3):
                to_peer(0, slot, c, d).wait_send()
            result(0, slot, d).wait_send()


def solution(mesh):
    n = mesh.shape["sp"]

    def body(x, gain, wq, wk, wv, wo):
        own, dim = x.shape
        per = n * HEAD
        stages = dim // per
        half = HEAD // 2
        angle = np.arange(n * own, dtype=np.float32)[:, None] * THETA ** (-np.arange(half, dtype=np.float32) / half)
        turns = jnp.asarray(np.concatenate([np.cos(angle), np.sin(angle)], 1).astype(np.float32))
        tokens = n * own
        low = jnp.bfloat16
        hbm = pl.BlockSpec(memory_space=pl.ANY)
        vmem = pl.BlockSpec(memory_space=pltpu.VMEM)
        return pl.pallas_call(
            functools.partial(_kernel, n),
            out_shape=pltpu.VMEM((own, dim), low),
            in_specs=[hbm, vmem, hbm, hbm, hbm, hbm, hbm],
            out_specs=vmem,
            scratch_shapes=[
                pltpu.VMEM((own, dim), low),
                pltpu.VMEM((RING, dim, WIDE), low),
                pltpu.VMEM((2, 3, n, own, HEAD), low),
                pltpu.VMEM((stages, 3, tokens, HEAD), low),
                pltpu.VMEM((2, tokens, HEAD), low),
                pltpu.VMEM((stages, own, per), low),
                pltpu.VMEM((own, dim), jnp.float32),
                pltpu.VMEM((tokens, STRIP), jnp.float32),
                pltpu.VMEM((tokens, STRIP), low),
                pltpu.VMEM((HEAD + 16, tokens), low),
                pltpu.VMEM((own, WIDE), low),
                pltpu.VMEM((2, 2, own, HEAD), jnp.float32),
                pltpu.VMEM((own, HEAD), jnp.float32),
                pltpu.SemaphoreType.DMA,
                pltpu.SemaphoreType.DMA,
                pltpu.SemaphoreType.DMA((RING,)),
                pltpu.SemaphoreType.DMA((2, 3, n)),
                pltpu.SemaphoreType.DMA((stages, 3, n)),
                pltpu.SemaphoreType.DMA((2, n)),
                pltpu.SemaphoreType.DMA((stages, n)),
            ],
            compiler_params=pltpu.CompilerParams(collective_id=0, has_side_effects=True, vmem_limit_bytes=62500000),
            name="layer",
        )(x, gain, turns, wq, wk, wv, wo)

    tokens, whole = P(("dp", "sp"), None), P(None, None)
    return jax.shard_map(
        body,
        mesh=mesh,
        in_specs=(tokens, P(None), whole, whole, whole, whole),
        out_specs=tokens,
        check_vma=False,
    )
```

```python
import functools

import jax
import jax.numpy as jnp
import numpy as np
from jax import lax
from jax.experimental import pallas as pl
from jax.experimental.pallas import tpu as pltpu
from jax.sharding import PartitionSpec as P

HEAD = 128
THETA = 10000
LOG2E = 1.4426950408889634
HIDDEN = -2e30
WIDE = 512
RING = 3
LAG = 1
STRIP = 512
PIECE = 64
ROWS = 64
MESH = pl.DeviceIdType.MESH


def _dot(a, b, ca, cb):
    return lax.dot_general(a, b, (((ca,), (cb,)), ((), ())), preferred_element_type=jnp.float32)


def _kernel(n, x_hbm, gain_ref, table_hbm, wq_hbm, wk_hbm, wv_hbm, wo_hbm, y_ref,
            a_ref, ring, sent, got, mine, seen, total, score, prob, vt, raw, table, turns,
            x_sem, table_sem, ring_sem, send_sem, recv_sem, osend_sem, orecv_sem):
    own, dim = a_ref.shape
    stages = got.shape[0]
    per = n * HEAD
    halves = per // WIDE
    heads = WIDE // HEAD
    ptiles = 3 * halves
    units = dim // per
    wtiles = dim // WIDE // units
    me = lax.axis_index("sp")
    scale = HEAD**-0.5 * LOG2E

    first_w = LAG + 1
    steps = stages + first_w
    head_tiles = first_w * ptiles
    mid_tiles = head_tiles + (stages - first_w) * (ptiles + wtiles)
    all_tiles = stages * (ptiles + wtiles)

    def fetch_p(slot, stage, i):
        for c, w in enumerate((wq_hbm, wk_hbm, wv_hbm)):
            for h in range(halves):
                @pl.when(i == c * halves + h)
                def _():
                    col = pl.multiple_of(stage * per + h * WIDE, WIDE)
                    pltpu.make_async_copy(w.at[:, pl.ds(col, WIDE)], ring.at[slot], ring_sem.at[slot]).start()

    def fetch_w(slot, stage, j):
        row = pl.multiple_of(stage * per, per)
        for u in range(units):
            col = pl.multiple_of((j * units + u) * WIDE, WIDE)
            pltpu.make_async_copy(wo_hbm.at[pl.ds(row, per), pl.ds(col, WIDE)], ring.at[slot, pl.ds(u * per, per)], ring_sem.at[slot]).start()

    def fetch(at):
        slot = lax.rem(at, RING)
        mid = jnp.maximum(at - head_tiles, 0)
        late = jnp.maximum(at - mid_tiles, 0)
        both = ptiles + wtiles
        in_head, in_mid = at < head_tiles, at < mid_tiles
        is_p = in_head | (in_mid & (lax.rem(mid, both) < ptiles))
        p_stage = jnp.where(in_head, lax.div(at, ptiles), first_w + lax.div(mid, both))
        p_tile = jnp.where(in_head, lax.rem(at, ptiles), lax.rem(mid, both))
        w_stage = jnp.where(in_mid, lax.div(mid, both), stages - first_w + lax.div(late, wtiles))
        w_tile = jnp.where(in_mid, lax.rem(mid, both) - ptiles, lax.rem(late, wtiles))

        @pl.when(is_p)
        def _():
            fetch_p(slot, p_stage, p_tile)

        @pl.when(jnp.logical_not(is_p) & (at < all_tiles))
        def _():
            fetch_w(slot, w_stage, w_tile)

    def arrived(at):
        slot = lax.rem(at, RING)
        pltpu.make_async_copy(wq_hbm.at[:, pl.ds(0, WIDE)], ring.at[slot], ring_sem.at[slot]).wait()
        return slot

    load_x = pltpu.make_async_copy(x_hbm, a_ref, x_sem)
    load_x.start()
    load_turns = pltpu.make_async_copy(table_hbm.at[pl.ds(pl.multiple_of(me * own, own), own)], turns, table_sem)
    load_turns.start()
    fetch_p(0, 0, 0)

    barrier = pltpu.get_barrier_semaphore()
    for k in range(1, n):
        pl.semaphore_signal(barrier, inc=1, device_id={"sp": lax.rem(me + k, n)}, device_id_type=MESH)

    vt[HEAD:, :] = jnp.ones((vt.shape[0] - HEAD, vt.shape[1]), vt.dtype)

    def clear(u, _):
        total[:, pl.ds(pl.multiple_of(u * WIDE, WIDE), WIDE)] = jnp.zeros((own, WIDE), jnp.float32)
        return 0

    lax.fori_loop(0, dim // WIDE, clear, 0)
    load_turns.wait()
    both_parts = turns[...]
    swapped = pltpu.roll(both_parts, HEAD // 2, 1)
    first = lax.broadcasted_iota(jnp.int32, both_parts.shape, 1) < HEAD // 2
    table[0, 0] = jnp.where(first, both_parts, swapped)
    table[0, 1] = jnp.where(first, -swapped, both_parts)
    table[1, 0] = jnp.ones_like(both_parts)
    table[1, 1] = jnp.zeros_like(both_parts)
    load_x.wait()
    for at in range(1, RING):
        fetch_p(at, 0, at)

    def norm(r, _):
        rows = pl.ds(pl.multiple_of(r * ROWS, ROWS), ROWS)
        squares = jnp.zeros((ROWS, HEAD), jnp.float32)
        for c in range(0, dim, HEAD):
            wide = a_ref[rows, c : c + HEAD].astype(jnp.float32)
            squares += wide * wide
        s = lax.rsqrt(squares.sum(-1, keepdims=True) / dim + 1e-6)
        s = jnp.broadcast_to(s, (ROWS, HEAD))
        for c in range(0, dim, HEAD):
            wide = a_ref[rows, c : c + HEAD].astype(jnp.float32)
            a_ref[rows, c : c + HEAD] = (wide * s * gain_ref[pl.ds(c, HEAD)].astype(jnp.float32).reshape(1, HEAD)).astype(a_ref.dtype)
        return 0

    lax.fori_loop(0, own // ROWS, norm, 0)
    pl.semaphore_wait(barrier, n - 1)

    def to_peer(stage, slot, c, d):
        return pltpu.make_async_remote_copy(
            src_ref=sent.at[slot, c, d], dst_ref=got.at[stage, c, pl.ds(pl.multiple_of(me * own, own), own)],
            send_sem=send_sem.at[slot, c, d], recv_sem=recv_sem.at[stage, c, me], device_id={"sp": d}, device_id_type=MESH)

    def result(stage, slot, d):
        return pltpu.make_async_remote_copy(
            src_ref=mine.at[slot, pl.ds(pl.multiple_of(d * own, own), own)], dst_ref=seen.at[stage, :, pl.ds(pl.multiple_of(me * HEAD, HEAD), HEAD)],
            send_sem=osend_sem.at[slot, d], recv_sem=orecv_sem.at[stage, me], device_id={"sp": d}, device_id_type=MESH)

    def base(t):
        return jnp.where(t < first_w, t * ptiles, head_tiles + jnp.minimum(t - first_w, stages - first_w) * (ptiles + wtiles)
                         + jnp.maximum(t - stages, 0) * wtiles)

    def project(t):
        slot = lax.rem(t, 2)

        @pl.when(t >= 2)
        def _():
            for c in range(3):
                for k in range(1, n):
                    to_peer(t, slot, c, lax.rem(me + k, n)).wait_send()

        def turn(c, h, to):
            for e in range(heads):
                v = raw[:, e * HEAD : (e + 1) * HEAD].astype(jnp.float32)
                cos, sin = table[lax.div(c, 2), 0], table[lax.div(c, 2), 1]
                sent[to, c, h * heads + e] = (v * cos + pltpu.roll(v, HEAD // 2, 1) * sin).astype(jnp.bfloat16)

        def send(c, h):
            for e in range(heads):
                d = h * heads + e

                @pl.when(d != me)
                def _():
                    to_peer(t, slot, c, d).start()

        def tile(i, _):
            at = base(t) + i
            w = arrived(at)
            before = jnp.maximum(i - 1, 0)
            c, h = lax.div(before, halves), lax.rem(before, halves)
            turn(c, h, jnp.where(t == 0, 1, slot))
            raw[...] = jnp.dot(a_ref[...], ring[w], preferred_element_type=jnp.float32).astype(jnp.bfloat16)
            fetch(at + RING)

            @pl.when((i > 0) & (t > 0))
            def _():
                send(c, h)

            @pl.when(t == 0)
            def _():
                now, part = lax.div(i, halves), lax.rem(i, halves)
                turn(now, part, 0)
                send(now, part)

            return 0

        lax.fori_loop(0, ptiles, tile, 0)

        @pl.when(t > 0)
        def _():
            turn(2, halves - 1, slot)
            send(2, halves - 1)

        for c in range(3):
            got[t, c, pl.ds(pl.multiple_of(me * own, own), own), :] = sent[slot, c, me]

    def attend(s):
        slot = lax.rem(s, 2)
        for c in range(3):
            for k in range(1, n):
                d = lax.rem(me + k, n)
                pltpu.make_async_remote_copy(
                    src_ref=sent.at[0, c, d], dst_ref=got.at[s, c, pl.ds(pl.multiple_of(d * own, own), own)], send_sem=send_sem.at[0, c, d],
                    recv_sem=recv_sem.at[s, c, d], device_id={"sp": d}, device_id_type=MESH).wait_recv()

        @pl.when(s >= 2)
        def _():
            for k in range(1, n):
                result(s, slot, lax.rem(me + k, n)).wait_send()

        tokens = n * own
        strips = tokens // STRIP
        for j in range(strips):
            here = slice(j * STRIP, (j + 1) * STRIP)
            vt[:HEAD, here] = got[s, 2, here, :].T
        gap = lax.broadcasted_iota(jnp.int32, (PIECE, STRIP), 1) - lax.broadcasted_iota(jnp.int32, (PIECE, STRIP), 0)

        def scores(i, j, top):
            q = got[s, 0, i * STRIP : (i + 1) * STRIP, :]
            one = _dot(got[s, 1, j * STRIP : (j + 1) * STRIP, :], q, 1, 1)
            for p in range(0, STRIP, PIECE):
                part = one[p : p + PIECE]
                if i == j:
                    part = jnp.where(gap >= p, part, HIDDEN)
                score[j * STRIP + p : j * STRIP + p + PIECE, :] = part
                high = part.reshape(PIECE // 8, 8, STRIP).max(axis=0)
                top = high if top is None else jnp.maximum(top, high)
            return top

        def weights(j, top):
            for p in range(j * STRIP, (j + 1) * STRIP, PIECE):
                prob[p : p + PIECE, :] = jnp.exp2((score[p : p + PIECE, :] - top) * scale).astype(jnp.bfloat16)

        def values(i):
            till = (i + 1) * STRIP
            mix = _dot(vt[:, :till], prob[:till, :], 1, 0)
            mine[slot, i * STRIP : till, :] = (mix[:HEAD] * (1 / mix[HEAD : HEAD + 1])).T.astype(jnp.bfloat16)

        top = scores(0, 0, None)
        for i in range(strips):
            top, after = top.max(axis=0, keepdims=True), None
            for j in range(i + 1):
                weights(j, top)
                if i + 1 < strips:
                    after = scores(i + 1, j, after)
            if i + 1 < strips:
                after = scores(i + 1, i + 1, after)
            values(i)
            top = after

        for d in range(n):
            @pl.when(d != me)
            def _():
                result(s, slot, d).start()

        seen[s, :, pl.ds(pl.multiple_of(me * HEAD, HEAD), HEAD)] = mine[slot, pl.ds(pl.multiple_of(me * own, own), own), :]

    def finish(t, s, last):
        if last:
            load_x.wait()

            def residual(r, _):
                rows = pl.ds(pl.multiple_of(r * 16, 16), 16)
                total[rows, :] += a_ref[rows, :].astype(jnp.float32)
                return 0

            lax.fori_loop(0, own // 16, residual, 0)
        for k in range(1, n):
            d = lax.rem(me + k, n)
            pltpu.make_async_remote_copy(
                src_ref=mine.at[0, pl.ds(0, own)], dst_ref=seen.at[s, :, pl.ds(pl.multiple_of(d * HEAD, HEAD), HEAD)],
                send_sem=osend_sem.at[0, d], recv_sem=orecv_sem.at[s, d], device_id={"sp": d}, device_id_type=MESH).wait_recv()

        def tile(j, _):
            at = base(t) + jnp.where(t < stages, ptiles, 0) + j
            w = arrived(at)
            for u in range(units):
                cols = pl.ds(pl.multiple_of((j * units + u) * WIDE, WIDE), WIDE)
                part = total[:, cols] + jnp.dot(seen[s], ring[w, u * per : (u + 1) * per, :], preferred_element_type=jnp.float32)
                if last:
                    y_ref[:, cols] = part.astype(y_ref.dtype)
                else:
                    total[:, cols] = part
            if not last:
                fetch(at + RING)
            return 0

        lax.fori_loop(0, wtiles, tile, 0)

    def step(t, _):
        @pl.when(t < stages)
        def _():
            project(t)

        @pl.when(t == stages)
        def _():
            load_x.start()

        @pl.when((t >= LAG) & (t < LAG + stages))
        def _():
            attend(t - LAG)

        @pl.when(t >= first_w)
        def _():
            finish(t, t - first_w, False)

        return 0

    lax.fori_loop(0, steps - 1, step, 0)
    finish(steps - 1, stages - 1, True)

    for slot in range(2):
        for k in range(1, n):
            d = lax.rem(me + k, n)
            for c in range(3):
                to_peer(0, slot, c, d).wait_send()
            result(0, slot, d).wait_send()


def solution(mesh):
    n = mesh.shape["sp"]

    def body(x, gain, wq, wk, wv, wo):
        own, dim = x.shape
        per = n * HEAD
        stages = dim // per
        half = HEAD // 2
        angle = np.arange(n * own, dtype=np.float32)[:, None] * THETA ** (-np.arange(half, dtype=np.float32) / half)
        turns = jnp.asarray(np.concatenate([np.cos(angle), np.sin(angle)], 1).astype(np.float32))
        tokens = n * own
        low = jnp.bfloat16
        hbm = pl.BlockSpec(memory_space=pl.ANY)
        vmem = pl.BlockSpec(memory_space=pltpu.VMEM)
        return pl.pallas_call(
            functools.partial(_kernel, n),
            out_shape=pltpu.VMEM((own, dim), low),
            in_specs=[hbm, vmem, hbm, hbm, hbm, hbm, hbm],
            out_specs=vmem,
            scratch_shapes=[
                pltpu.VMEM((own, dim), low),
                pltpu.VMEM((RING, dim, WIDE), low),
                pltpu.VMEM((2, 3, n, own, HEAD), low),
                pltpu.VMEM((stages, 3, tokens, HEAD), low),
                pltpu.VMEM((2, tokens, HEAD), low),
                pltpu.VMEM((stages, own, per), low),
                pltpu.VMEM((own, dim), jnp.float32),
                pltpu.VMEM((tokens, STRIP), jnp.float32),
                pltpu.VMEM((tokens, STRIP), low),
                pltpu.VMEM((HEAD + 16, tokens), low),
                pltpu.VMEM((own, WIDE), low),
                pltpu.VMEM((2, 2, own, HEAD), jnp.float32),
                pltpu.VMEM((own, HEAD), jnp.float32),
                pltpu.SemaphoreType.DMA,
                pltpu.SemaphoreType.DMA,
                pltpu.SemaphoreType.DMA((RING,)),
                pltpu.SemaphoreType.DMA((2, 3, n)),
                pltpu.SemaphoreType.DMA((stages, 3, n)),
                pltpu.SemaphoreType.DMA((2, n)),
                pltpu.SemaphoreType.DMA((stages, n)),
            ],
            compiler_params=pltpu.CompilerParams(collective_id=0, has_side_effects=True, vmem_limit_bytes=62500000),
            name="layer",
        )(x, gain, turns, wq, wk, wv, wo)

    tokens, whole = P(("dp", "sp"), None), P(None, None)
    return jax.shard_map(
        body,
        mesh=mesh,
        in_specs=(tokens, P(None), whole, whole, whole, whole),
        out_specs=tokens,
        check_vma=False,
    )
```

```python
import functools

import jax
import jax.numpy as jnp
import numpy as np
from jax import lax
from jax.experimental import pallas as pl
from jax.experimental.pallas import tpu as pltpu
from jax.sharding import PartitionSpec as P

HEAD = 128
THETA = 10000
LOG2E = 1.4426950408889634
HIDDEN = -2e30
WIDE = 512
RING = 3
LAG = 1
STRIP = 512
PIECE = 64
ROWS = 64
MESH = pl.DeviceIdType.MESH


def _dot(a, b, ca, cb):
    return lax.dot_general(a, b, (((ca,), (cb,)), ((), ())), preferred_element_type=jnp.float32)


def _kernel(n, x_hbm, gain_ref, table_hbm, wq_hbm, wk_hbm, wv_hbm, wo_hbm, y_ref,
            a_ref, ring, sent, got, mine, seen, total, score, prob, vt, raw, table, turns,
            x_sem, table_sem, ring_sem, send_sem, recv_sem, osend_sem, orecv_sem):
    own, dim = a_ref.shape
    stages = got.shape[0]
    per = n * HEAD
    halves = per // WIDE
    heads = WIDE // HEAD
    ptiles = 3 * halves
    units = dim // per
    wtiles = dim // WIDE // units
    me = lax.axis_index("sp")
    scale = HEAD**-0.5 * LOG2E

    first_w = LAG + 1
    steps = stages + first_w
    head_tiles = first_w * ptiles
    mid_tiles = head_tiles + (stages - first_w) * (ptiles + wtiles)
    all_tiles = stages * (ptiles + wtiles)

    def fetch_p(slot, stage, i):
        for c, w in enumerate((wq_hbm, wk_hbm, wv_hbm)):
            for h in range(halves):
                @pl.when(i == c * halves + h)
                def _():
                    col = pl.multiple_of(stage * per + h * WIDE, WIDE)
                    pltpu.make_async_copy(w.at[:, pl.ds(col, WIDE)], ring.at[slot], ring_sem.at[slot]).start()

    def fetch_w(slot, stage, j):
        row = pl.multiple_of(stage * per, per)
        for u in range(units):
            col = pl.multiple_of((j * units + u) * WIDE, WIDE)
            pltpu.make_async_copy(wo_hbm.at[pl.ds(row, per), pl.ds(col, WIDE)], ring.at[slot, pl.ds(u * per, per)], ring_sem.at[slot]).start()

    def fetch(at):
        slot = lax.rem(at, RING)
        mid = jnp.maximum(at - head_tiles, 0)
        late = jnp.maximum(at - mid_tiles, 0)
        both = ptiles + wtiles
        in_head, in_mid = at < head_tiles, at < mid_tiles
        is_p = in_head | (in_mid & (lax.rem(mid, both) < ptiles))
        p_stage = jnp.where(in_head, lax.div(at, ptiles), first_w + lax.div(mid, both))
        p_tile = jnp.where(in_head, lax.rem(at, ptiles), lax.rem(mid, both))
        w_stage = jnp.where(in_mid, lax.div(mid, both), stages - first_w + lax.div(late, wtiles))
        w_tile = jnp.where(in_mid, lax.rem(mid, both) - ptiles, lax.rem(late, wtiles))

        @pl.when(is_p)
        def _():
            fetch_p(slot, p_stage, p_tile)

        @pl.when(jnp.logical_not(is_p) & (at < all_tiles))
        def _():
            fetch_w(slot, w_stage, w_tile)

    def arrived(at):
        slot = lax.rem(at, RING)
        pltpu.make_async_copy(wq_hbm.at[:, pl.ds(0, WIDE)], ring.at[slot], ring_sem.at[slot]).wait()
        return slot

    load_x = pltpu.make_async_copy(x_hbm, a_ref, x_sem)
    load_x.start()
    load_turns = pltpu.make_async_copy(table_hbm.at[pl.ds(pl.multiple_of(me * own, own), own)], turns, table_sem)
    load_turns.start()
    fetch_p(0, 0, 0)

    barrier = pltpu.get_barrier_semaphore()
    for k in range(1, n):
        pl.semaphore_signal(barrier, inc=1, device_id={"sp": lax.rem(me + k, n)}, device_id_type=MESH)

    vt[HEAD:, :] = jnp.ones((vt.shape[0] - HEAD, vt.shape[1]), vt.dtype)

    def clear(u, _):
        total[:, pl.ds(pl.multiple_of(u * WIDE, WIDE), WIDE)] = jnp.zeros((own, WIDE), jnp.float32)
        return 0

    lax.fori_loop(0, dim // WIDE, clear, 0)
    load_turns.wait()
    both_parts = turns[...]
    swapped = pltpu.roll(both_parts, HEAD // 2, 1)
    first = lax.broadcasted_iota(jnp.int32, both_parts.shape, 1) < HEAD // 2
    table[0, 0] = jnp.where(first, both_parts, swapped)
    table[0, 1] = jnp.where(first, -swapped, both_parts)
    table[1, 0] = jnp.ones_like(both_parts)
    table[1, 1] = jnp.zeros_like(both_parts)
    load_x.wait()
    for at in range(1, RING):
        fetch_p(at, 0, at)

    def norm(r, _):
        rows = pl.ds(pl.multiple_of(r * ROWS, ROWS), ROWS)
        squares = jnp.zeros((ROWS, HEAD), jnp.float32)
        for c in range(0, dim, HEAD):
            wide = a_ref[rows, c : c + HEAD].astype(jnp.float32)
            squares += wide * wide
        s = lax.rsqrt(squares.sum(-1, keepdims=True) / dim + 1e-6)
        s = jnp.broadcast_to(s, (ROWS, HEAD))
        for c in range(0, dim, HEAD):
            wide = a_ref[rows, c : c + HEAD].astype(jnp.float32)
            a_ref[rows, c : c + HEAD] = (wide * s * gain_ref[pl.ds(c, HEAD)].astype(jnp.float32).reshape(1, HEAD)).astype(a_ref.dtype)
        return 0

    lax.fori_loop(0, own // ROWS, norm, 0)
    pl.semaphore_wait(barrier, n - 1)

    def whose(head):
        return lax.rem(head, n // 2) * 2 + lax.div(head, n // 2)

    def place(device):
        return lax.rem(device, 2) * (n // 2) + lax.div(device, 2)

    def to_peer(stage, slot, c, d):
        return pltpu.make_async_remote_copy(
            src_ref=sent.at[slot, c, place(d)], dst_ref=got.at[stage, c, pl.ds(pl.multiple_of(me * own, own), own)],
            send_sem=send_sem.at[slot, c, d], recv_sem=recv_sem.at[stage, c, me], device_id={"sp": d}, device_id_type=MESH)

    def result(stage, slot, d):
        return pltpu.make_async_remote_copy(
            src_ref=mine.at[slot, pl.ds(pl.multiple_of(d * own, own), own)], dst_ref=seen.at[stage, :, pl.ds(pl.multiple_of(place(me) * HEAD, HEAD), HEAD)],
            send_sem=osend_sem.at[slot, d], recv_sem=orecv_sem.at[stage, me], device_id={"sp": d}, device_id_type=MESH)

    def base(t):
        return jnp.where(t < first_w, t * ptiles, head_tiles + jnp.minimum(t - first_w, stages - first_w) * (ptiles + wtiles)
                         + jnp.maximum(t - stages, 0) * wtiles)

    def project(t):
        slot = lax.rem(t, 2)

        @pl.when(t >= 2)
        def _():
            for c in range(3):
                for k in range(1, n):
                    to_peer(t, slot, c, lax.rem(me + k, n)).wait_send()

        def turn(c, h, to):
            for e in range(heads):
                v = raw[:, e * HEAD : (e + 1) * HEAD].astype(jnp.float32)
                cos, sin = table[lax.div(c, 2), 0], table[lax.div(c, 2), 1]
                sent[to, c, h * heads + e] = (v * cos + pltpu.roll(v, HEAD // 2, 1) * sin).astype(jnp.bfloat16)

        def send(c, h):
            for e in range(heads):
                d = whose(h * heads + e)

                @pl.when(d != me)
                def _():
                    to_peer(t, slot, c, d).start()

        def tile(i, _):
            at = base(t) + i
            w = arrived(at)
            before = jnp.maximum(i - 1, 0)
            c, h = lax.div(before, halves), lax.rem(before, halves)
            turn(c, h, jnp.where(t == 0, 1, slot))
            raw[...] = jnp.dot(a_ref[...], ring[w], preferred_element_type=jnp.float32).astype(jnp.bfloat16)
            fetch(at + RING)

            @pl.when((i > 0) & (t > 0))
            def _():
                send(c, h)

            @pl.when(t == 0)
            def _():
                now, part = lax.div(i, halves), lax.rem(i, halves)
                turn(now, part, 0)
                send(now, part)

            return 0

        lax.fori_loop(0, ptiles, tile, 0)

        @pl.when(t > 0)
        def _():
            turn(2, halves - 1, slot)
            send(2, halves - 1)

        for c in range(3):
            got[t, c, pl.ds(pl.multiple_of(me * own, own), own), :] = sent[slot, c, place(me)]

    def attend(s):
        slot = lax.rem(s, 2)
        for c in range(3):
            for k in range(1, n):
                d = lax.rem(me + k, n)
                pltpu.make_async_remote_copy(
                    src_ref=sent.at[0, c, d], dst_ref=got.at[s, c, pl.ds(pl.multiple_of(d * own, own), own)], send_sem=send_sem.at[0, c, d],
                    recv_sem=recv_sem.at[s, c, d], device_id={"sp": d}, device_id_type=MESH).wait_recv()

        @pl.when(s >= 2)
        def _():
            for k in range(1, n):
                result(s, slot, lax.rem(me + k, n)).wait_send()

        tokens = n * own
        strips = tokens // STRIP
        for j in range(strips):
            here = slice(j * STRIP, (j + 1) * STRIP)
            vt[:HEAD, here] = got[s, 2, here, :].T
        gap = lax.broadcasted_iota(jnp.int32, (PIECE, STRIP), 1) - lax.broadcasted_iota(jnp.int32, (PIECE, STRIP), 0)

        def scores(i, j, top):
            q = got[s, 0, i * STRIP : (i + 1) * STRIP, :]
            one = _dot(got[s, 1, j * STRIP : (j + 1) * STRIP, :], q, 1, 1)
            for p in range(0, STRIP, PIECE):
                part = one[p : p + PIECE]
                if i == j:
                    part = jnp.where(gap >= p, part, HIDDEN)
                score[j * STRIP + p : j * STRIP + p + PIECE, :] = part
                high = part.reshape(PIECE // 8, 8, STRIP).max(axis=0)
                top = high if top is None else jnp.maximum(top, high)
            return top

        def weights(j, top):
            for p in range(j * STRIP, (j + 1) * STRIP, PIECE):
                prob[p : p + PIECE, :] = jnp.exp2((score[p : p + PIECE, :] - top) * scale).astype(jnp.bfloat16)

        def values(i):
            till = (i + 1) * STRIP
            mix = _dot(vt[:, :till], prob[:till, :], 1, 0)
            mine[slot, i * STRIP : till, :] = (mix[:HEAD] * (1 / mix[HEAD : HEAD + 1])).T.astype(jnp.bfloat16)

        top = scores(0, 0, None)
        for i in range(strips):
            top, after = top.max(axis=0, keepdims=True), None
            for j in range(i + 1):
                weights(j, top)
                if i + 1 < strips:
                    after = scores(i + 1, j, after)
            if i + 1 < strips:
                after = scores(i + 1, i + 1, after)
            values(i)
            top = after

        for d in range(n):
            @pl.when(d != me)
            def _():
                result(s, slot, d).start()

        seen[s, :, pl.ds(pl.multiple_of(place(me) * HEAD, HEAD), HEAD)] = mine[slot, pl.ds(pl.multiple_of(me * own, own), own), :]

    def finish(t, s, last):
        if last:
            load_x.wait()

            def residual(r, _):
                rows = pl.ds(pl.multiple_of(r * 16, 16), 16)
                total[rows, :] += a_ref[rows, :].astype(jnp.float32)
                return 0

            lax.fori_loop(0, own // 16, residual, 0)
        for k in range(1, n):
            d = lax.rem(me + k, n)
            pltpu.make_async_remote_copy(
                src_ref=mine.at[0, pl.ds(0, own)], dst_ref=seen.at[s, :, pl.ds(pl.multiple_of(place(d) * HEAD, HEAD), HEAD)],
                send_sem=osend_sem.at[0, d], recv_sem=orecv_sem.at[s, d], device_id={"sp": d}, device_id_type=MESH).wait_recv()

        def tile(j, _):
            at = base(t) + jnp.where(t < stages, ptiles, 0) + j
            w = arrived(at)
            for u in range(units):
                cols = pl.ds(pl.multiple_of((j * units + u) * WIDE, WIDE), WIDE)
                part = total[:, cols] + jnp.dot(seen[s], ring[w, u * per : (u + 1) * per, :], preferred_element_type=jnp.float32)
                if last:
                    y_ref[:, cols] = part.astype(y_ref.dtype)
                else:
                    total[:, cols] = part
            if not last:
                fetch(at + RING)
            return 0

        lax.fori_loop(0, wtiles, tile, 0)

    def step(t, _):
        @pl.when(t < stages)
        def _():
            project(t)

        @pl.when(t == stages)
        def _():
            load_x.start()

        @pl.when((t >= LAG) & (t < LAG + stages))
        def _():
            attend(t - LAG)

        @pl.when(t >= first_w)
        def _():
            finish(t, t - first_w, False)

        return 0

    lax.fori_loop(0, steps - 1, step, 0)
    finish(steps - 1, stages - 1, True)

    for slot in range(2):
        for k in range(1, n):
            d = lax.rem(me + k, n)
            for c in range(3):
                to_peer(0, slot, c, d).wait_send()
            result(0, slot, d).wait_send()


def solution(mesh):
    n = mesh.shape["sp"]

    def body(x, gain, wq, wk, wv, wo):
        own, dim = x.shape
        per = n * HEAD
        stages = dim // per
        half = HEAD // 2
        angle = np.arange(n * own, dtype=np.float32)[:, None] * THETA ** (-np.arange(half, dtype=np.float32) / half)
        turns = jnp.asarray(np.concatenate([np.cos(angle), np.sin(angle)], 1).astype(np.float32))
        tokens = n * own
        low = jnp.bfloat16
        hbm = pl.BlockSpec(memory_space=pl.ANY)
        vmem = pl.BlockSpec(memory_space=pltpu.VMEM)
        return pl.pallas_call(
            functools.partial(_kernel, n),
            out_shape=pltpu.VMEM((own, dim), low),
            in_specs=[hbm, vmem, hbm, hbm, hbm, hbm, hbm],
            out_specs=vmem,
            scratch_shapes=[
                pltpu.VMEM((own, dim), low),
                pltpu.VMEM((RING, dim, WIDE), low),
                pltpu.VMEM((2, 3, n, own, HEAD), low),
                pltpu.VMEM((stages, 3, tokens, HEAD), low),
                pltpu.VMEM((2, tokens, HEAD), low),
                pltpu.VMEM((stages, own, per), low),
                pltpu.VMEM((own, dim), jnp.float32),
                pltpu.VMEM((tokens, STRIP), jnp.float32),
                pltpu.VMEM((tokens, STRIP), low),
                pltpu.VMEM((HEAD + 16, tokens), low),
                pltpu.VMEM((own, WIDE), low),
                pltpu.VMEM((2, 2, own, HEAD), jnp.float32),
                pltpu.VMEM((own, HEAD), jnp.float32),
                pltpu.SemaphoreType.DMA,
                pltpu.SemaphoreType.DMA,
                pltpu.SemaphoreType.DMA((RING,)),
                pltpu.SemaphoreType.DMA((2, 3, n)),
                pltpu.SemaphoreType.DMA((stages, 3, n)),
                pltpu.SemaphoreType.DMA((2, n)),
                pltpu.SemaphoreType.DMA((stages, n)),
            ],
            compiler_params=pltpu.CompilerParams(collective_id=0, has_side_effects=True, vmem_limit_bytes=62500000),
            name="layer",
        )(x, gain, turns, wq, wk, wv, wo)

    tokens, whole = P(("dp", "sp"), None), P(None, None)
    return jax.shard_map(
        body,
        mesh=mesh,
        in_specs=(tokens, P(None), whole, whole, whole, whole),
        out_specs=tokens,
        check_vma=False,
    )
```
